512 devices in a mesh: cuts: 32 (over z, y_hi, core), row: 16 (over x, y_lo).
Axes of the slice: x: 4, y: 8 (y_hi: 2, y_lo: 4; y = y_hi * 4 + y_lo), z: 8, core: 2. Of those that a mesh axis runs over, the one named last changes fastest.
Arguments:
- propagator: float32 [8192, 8192], P('row', 'cuts'), as said below
- slab: float32 [8192, 256], P('cuts', 'row'), may hold values from -6 to 6
- fields: int32 [4, 8192], replicated, may hold values from 0 to 1
- phonon: int32 [4, 8192], replicated, may hold values from 0 to 15
- couplings: float32 [16], replicated, may hold values from -0.6 to 0.6
Outputs:
- updated: float32 [8192, 256], P('cuts', 'row')
The draws below stay inside these ranges and needn't reach their ends.
Inputs may be any that keep to these rules, and one draw needn't show every extreme that they name: propagator is symmetric.
All inputs are finite; a program needn't handle non-finite values.
Results may differ from the reference program's by a relative error of at most 0.00011.
Values sent between devices are 32-bit elements; how exact they have to be, the bound alone decides.
No kernel may reach another device: no remote copies, remote signals or barrier semaphores. Data moves between devices by JAX's collectives and lax.ppermute only.
A program may use at most 64 MiB of HBM per device.

```python
import math
import jax
import jax.numpy as jnp
from jax import lax

SITES = 8192
SLAB = 256
SLICES = 4
LEVELS = 16


def draw_propagator(key, part):
    noise = jax.random.normal(key, (SITES, SITES), jnp.float32)
    symmetric = (noise + noise.T) * (0.25 / math.sqrt(2.0 * SITES))
    return symmetric + jnp.eye(SITES, dtype=jnp.float32)


def touch_ends(values, own_key, least, high):
    index_at = [jax.random.randint(jax.random.fold_in(own_key, axis), (), 0, length) for axis, length in enumerate(values.shape)]
    main_axis = values.shape.index(max(values.shape))
    next_to = index_at[:main_axis] + [(index_at[main_axis] + 1) % values.shape[main_axis]] + index_at[main_axis + 1:]
    return values.at[tuple(index_at)].set(least).at[tuple(next_to)].set(high)


def block_scale(stream_key, shape, shards, least, top_value):
    factor_of = 1.0
    for position, blocks in shards:
        draws = jax.random.uniform(jax.random.fold_in(jax.random.fold_in(stream_key, 6), position), (blocks,), jnp.float32, least / len(shards), top_value / len(shards))
        factor_of = factor_of * jnp.repeat(jnp.exp(draws), shape[position] // blocks).reshape((-1,) + (1,) * (len(shape) - 1 - position))
    return factor_of


def bell_draw(key, dims, deviation, most, pieces=(), held_as=jnp.bfloat16):
    result = jax.random.normal(key, dims, jnp.float32) * deviation
    if len(pieces) > 0:
        result = block_scale(key, dims, pieces, -0.22, 0.18) * result
    return jnp.clip(result, min=-most, max=most).astype(held_as)


def setup_inputs(seed: int = 0) -> dict:
    arg_keys = jax.random.split(jax.random.key(seed), 6)
    propagator = draw_propagator(jax.random.fold_in(arg_keys[5], 71), 0)
    slab = bell_draw(arg_keys[1], (SITES, SLAB), 1.0, 6.0, ((0, 32), (1, 16)), jnp.float32)
    fields = touch_ends(jax.random.randint(arg_keys[2], (SLICES, SITES), 0, 2), jax.random.fold_in(arg_keys[2], 1), 0, 1).astype(jnp.int32)
    phonon = touch_ends(jax.random.randint(arg_keys[3], (SLICES, SITES), 0, LEVELS), jax.random.fold_in(arg_keys[3], 1), 0, LEVELS - 1).astype(jnp.int32)
    couplings = jnp.clip(jax.random.uniform(arg_keys[4], (LEVELS,), jnp.float32, -0.6, 0.6), -0.6, 0.6)
    return {"propagator": propagator, "slab": slab, "fields": fields, "phonon": phonon, "couplings": couplings}


def reference(propagator, slab, fields, phonon, couplings):
    sites = jnp.arange(SITES).astype(jnp.int32)
    parity = sites % 2
    current = slab
    for slice_no in range(SLICES):
        mixed = jnp.dot(propagator, current, precision=lax.Precision.HIGHEST, preferred_element_type=jnp.float32)
        rates = couplings[phonon[slice_no]]
        even_rate = rates[sites - parity][:, None]
        odd_rate = rates[(sites - 1 + parity + SITES) % SITES][:, None]
        partner = jnp.where(parity[:, None] == 0, jnp.roll(mixed, -1, 0), jnp.roll(mixed, 1, 0))
        mixed = jnp.cosh(even_rate) * mixed + jnp.sinh(even_rate) * partner
        partner = jnp.where(parity[:, None] == 0, jnp.roll(mixed, 1, 0), jnp.roll(mixed, -1, 0))
        mixed = jnp.cosh(odd_rate) * mixed + jnp.sinh(odd_rate) * partner
        signs = (2 * fields[slice_no] - 1).astype(jnp.float32)
        current = jnp.exp(0.3 * signs)[:, None] * mixed
    return current
```

```python
import functools

import jax
import jax.numpy as jnp
from jax import lax
from jax.experimental import pallas as pl
from jax.experimental.pallas import tpu as pltpu
from jax.sharding import Mesh, PartitionSpec as P

SITES = 8192
SLICES = 4

hs_strength = 0.3

ROW = ("x", "ylo")
CUT = ("z", "yhi")


def twin(x):
    return lax.ppermute(x, "core", [(0, 1), (1, 0)])


def shifted(x, axes, step):
    count = lax.axis_size(axes)
    return lax.ppermute(x, axes, [(i, (i + step) % count) for i in range(count)])


def exchanged(parts, axes):
    return lax.all_to_all(parts, axes, 0, 0, tiled=True)


def gathered(x, axes):
    count = lax.axis_size(axes)
    parts = exchanged(jnp.broadcast_to(x[None], (count, *x.shape)), axes)
    return parts.reshape(count * x.shape[0], x.shape[1])


def summed(x, axes):
    count = lax.axis_size(axes)
    return exchanged(x.reshape(count, x.shape[0] // count, x.shape[1]), axes).sum(axis=0)


def lookup(indices, couplings):
    levels = jnp.arange(couplings.shape[0], dtype=jnp.int32)
    hits = indices[None, :] == levels[:, None]
    return jnp.sum(jnp.where(hits, couplings[:, None], 0.0), axis=0)


def mixing(slice_no, first, count, fields, phonon, couplings):
    levels = phonon[slice_no]
    window = lax.dynamic_slice_in_dim(levels, first, count)
    before = lax.dynamic_slice_in_dim(levels, (first - 2 + SITES) % SITES, 2)
    after = lax.dynamic_slice_in_dim(levels, (first + count) % SITES, 2)
    rate = lookup(window, couplings)
    edge = lookup(jnp.concatenate([before, after]), couplings)
    even = jnp.arange(count, dtype=jnp.int32) % 2 == 0
    left = jnp.concatenate([edge[1:2], rate[:-1]])
    even_rate = jnp.where(even, rate, left)
    odd_rate = jnp.where(even, left, rate)
    signs = (2 * lax.dynamic_slice_in_dim(fields[slice_no], first, count) - 1).astype(jnp.float32)
    scale = jnp.exp(hs_strength * signs)
    outer = jnp.concatenate([edge[0:1], edge[2:3]])
    outer = jnp.concatenate([jnp.cosh(outer), jnp.sinh(outer)])
    outer = jnp.pad(outer, (0, count - 4))
    zero = jnp.zeros_like(rate)
    return jnp.stack(
        [
            jnp.cosh(even_rate),
            jnp.sinh(even_rate),
            scale * jnp.cosh(odd_rate),
            scale * jnp.sinh(odd_rate),
            outer,
            zero,
            zero,
            zero,
        ]
    )


def halves(x):
    high = x.astype(jnp.bfloat16)
    return high, (x - high.astype(jnp.float32)).astype(jnp.bfloat16)


def product(a, b, contract_b):
    dims = (((1,), (contract_b,)), ((), ()))
    dot = functools.partial(lax.dot_general, dimension_numbers=dims, preferred_element_type=jnp.float32)
    a_high, a_low = halves(a)
    b_high, b_low = halves(b)
    return dot(a_high, b_high) + (dot(a_high, b_low) + dot(a_low, b_high))


def slice_kernel(across, core_ref, u_ref, mine_ref, other_ref, rim_ref, mix_ref, out_ref, w_ref):
    width = mine_ref.shape[1]
    core = core_ref[0]
    at_mine = pl.ds(pl.multiple_of(core * width, width), width)
    at_other = pl.ds(pl.multiple_of((1 - core) * width, width), width)
    mix = mix_ref[...]
    rim = rim_ref[...]
    rim_left = mix[4:5, 2:3] * rim[0:1] + mix[4:5, 0:1] * rim[1:2]
    rim_right = mix[4:5, 1:2] * rim[2:3] + mix[4:5, 3:4] * rim[3:4]
    if across:
        u_mine, u_other = u_ref[:, at_mine], u_ref[:, at_other]
        w = product(u_mine, mine_ref[...], 1) + product(u_other, other_ref[...], 1)
        u = jnp.concatenate([u_mine, u_other], axis=1)
    else:
        u = u_ref[...]
        w_ref[:, at_mine] = product(u, mine_ref[...], 0)
        w_ref[:, at_other] = product(u, other_ref[...], 0)
        w = w_ref[...]
    end_left = jnp.sum(u * rim_left, axis=1, keepdims=True)
    end_right = jnp.sum(u * rim_right, axis=1, keepdims=True)
    count = w.shape[1]
    lane = lax.broadcasted_iota(jnp.int32, w.shape, 1)
    even = lane % 2 == 0
    partner = jnp.where(even, pltpu.roll(w, count - 1, 1), pltpu.roll(w, 1, 1))
    e = mix[0:1] * w + mix[1:2] * partner
    below = jnp.where(lane == 0, end_left, pltpu.roll(e, 1, 1))
    above = jnp.where(lane == count - 1, end_right, pltpu.roll(e, count - 1, 1))
    out_ref[...] = mix[2:3] * e + mix[3:4] * jnp.where(even, below, above)


def one_slice(across, core, u, mine, other, rim, mix):
    columns, depth = u.shape
    sites = mine.shape[0] if across else 2 * mine.shape[1]
    vmem = pl.BlockSpec(memory_space=pltpu.VMEM)
    return pl.pallas_call(
        functools.partial(slice_kernel, across),
        out_shape=jax.ShapeDtypeStruct((columns, sites), jnp.float32),
        in_specs=[pl.BlockSpec(memory_space=pltpu.SMEM)] + [vmem] * 5,
        out_specs=vmem,
        scratch_shapes=[pltpu.VMEM((columns, sites), jnp.float32)],
        compiler_params=pltpu.CompilerParams(vmem_limit_bytes=24 * 1024 * 1024),
        cost_estimate=pl.CostEstimate(
            flops=12 * columns * depth * sites, bytes_accessed=8 * depth * sites, transcendentals=0
        ),
        name="across" if across else "along",
    )(core, u, mine, other, rim, mix)


def shards(propagator, slab, fields, phonon, couplings):
    core = lax.axis_index("core")
    first_core = core == 0
    columns = slab.T
    half = columns.shape[0] // 2
    near = columns.shape[1]

    kept = lax.dynamic_slice_in_dim(columns, core * half, half, axis=0)
    given = lax.dynamic_slice_in_dim(columns, (1 - core) * half, half, axis=0)
    taken = twin(given)
    both = jnp.where(first_core, jnp.concatenate([kept, taken], 1), jnp.concatenate([taken, kept], 1))
    u = gathered(both, ROW)

    mine = propagator
    other = twin(propagator)
    block = mine.shape[0]
    count = 2 * mine.shape[1]

    def rims(low, high, axes):
        before = shifted(high, axes, 1)
        after = shifted(low, axes, -1)
        return jnp.concatenate([before, after, jnp.zeros((4, before.shape[1]), jnp.float32)], axis=0)

    row_rim = rims(
        jnp.concatenate([mine[:2], other[:2]], axis=1),
        jnp.concatenate([mine[-2:], other[-2:]], axis=1),
        ROW,
    )
    first = jnp.where(first_core, mine[:, :2], other[:, :2]).T
    last = jnp.where(first_core, other[:, -2:], mine[:, -2:]).T
    cut_rim = rims(first, last, CUT)

    row_first = lax.axis_index(ROW) * block
    cut_first = lax.axis_index(CUT) * count
    which = jnp.reshape(core, (1,)).astype(jnp.int32)
    for slice_no in range(SLICES):
        across = slice_no % 2 == 0
        if across:
            mix = mixing(slice_no, row_first, block, fields, phonon, couplings)
        else:
            mix = mixing(slice_no, cut_first, count, fields, phonon, couplings)
        w = one_slice(across, which, u, mine, other, row_rim if across else cut_rim, mix)
        axes = CUT if across else ROW
        share = summed(w, axes)
        if slice_no < SLICES - 1:
            u = gathered(share, axes)
    kept = lax.dynamic_slice_in_dim(share, core * near, near, axis=1)
    given = lax.dynamic_slice_in_dim(share, (1 - core) * near, near, axis=1)
    taken = twin(given)
    out = jnp.where(first_core, jnp.concatenate([kept, taken], 0), jnp.concatenate([taken, kept], 0))
    return out.T


def solution(mesh):
    devices = mesh.devices.reshape(8, 2, 2, 4, 4)
    fine = Mesh(devices, ("z", "yhi", "core", "x", "ylo"))
    cuts, row = ("z", "yhi", "core"), ROW
    in_specs = (P(row, cuts), P(cuts, row), P(), P(), P())
    return jax.shard_map(shards, mesh=fine, in_specs=in_specs, out_specs=P(cuts, row), check_vma=False)
```

```python
import functools

import jax
import jax.numpy as jnp
from jax import lax
from jax.experimental import pallas as pl
from jax.experimental.pallas import tpu as pltpu
from jax.sharding import Mesh, PartitionSpec as P

SITES = 8192
SLICES = 4
LEVELS = 16
LANES = 128

hs_strength = 0.3

ROW = ("x", "ylo")
CUT = ("z", "yhi")
PAIRED_ROW = ("core", "x", "ylo")

VMEM = pl.BlockSpec(memory_space=pltpu.VMEM)
SMEM = pl.BlockSpec(memory_space=pltpu.SMEM)


def swapped(x, axis):
    return lax.ppermute(x, axis, [(0, 1), (1, 0)])


def exchanged(parts, axes):
    return lax.all_to_all(parts, axes, 0, 0, tiled=True)


def gathered(x, axes):
    count = lax.axis_size(axes)
    parts = exchanged(jnp.broadcast_to(x[None], (count, *x.shape)), axes)
    return parts.reshape(count * x.shape[0], x.shape[1])


def summed(x, axes):
    count = lax.axis_size(axes)
    return exchanged(x.reshape(count, x.shape[0] // count, x.shape[1]), axes).sum(axis=0)


def call(kernel, name, out_shape, in_specs, scratch=(), flops=0, size=0):
    return pl.pallas_call(
        kernel,
        out_shape=out_shape,
        in_specs=in_specs,
        out_specs=jax.tree.map(lambda _: VMEM, out_shape),
        scratch_shapes=list(scratch),
        compiler_params=pltpu.CompilerParams(vmem_limit_bytes=24 * 1024 * 1024),
        cost_estimate=pl.CostEstimate(flops=flops, bytes_accessed=size, transcendentals=0),
        name=name,
    )


def mixing_kernel(first_ref, couplings_ref, phonon_ref, fields_ref, out_ref):
    count = out_ref.shape[2]
    for turn in range(2):
        first = first_ref[turn]
        at_before = pl.ds(pl.multiple_of((first + (SITES - LANES)) % SITES, LANES), LANES)
        at_block = pl.ds(pl.multiple_of(first, LANES), count)
        at_after = pl.ds(pl.multiple_of((first + count) % SITES, LANES), LANES)
        level = jnp.concatenate([phonon_ref[:, at_before], phonon_ref[:, at_block], phonon_ref[:, at_after]], axis=1)
        rate = jnp.zeros(level.shape, jnp.float32)
        for k in range(LEVELS):
            rate = jnp.where(level == k, couplings_ref[k], rate)
        grown, shrunk = jnp.exp(rate), jnp.exp(-rate)
        cosh, sinh = 0.5 * (grown + shrunk), 0.5 * (grown - shrunk)
        cosh_left, sinh_left = pltpu.roll(cosh, 1, 1), pltpu.roll(sinh, 1, 1)
        even = lax.broadcasted_iota(jnp.int32, rate.shape, 1) % 2 == 0
        inside = slice(LANES, LANES + count)
        sign = (2 * fields_ref[:, at_block] - 1).astype(jnp.float32)
        scale = jnp.exp(hs_strength * sign)
        rows = [
            jnp.where(even, cosh, cosh_left)[:, inside],
            jnp.where(even, sinh, sinh_left)[:, inside],
            scale * jnp.where(even, cosh_left, cosh)[:, inside],
            scale * jnp.where(even, sinh_left, sinh)[:, inside],
            jnp.concatenate(
                [cosh[:, :LANES], cosh[:, LANES + count :], sinh[:, :LANES], sinh[:, LANES + count :]], axis=1
            ),
        ]
        for slice_no in range(turn, SLICES, 2):
            for k, row in enumerate(rows):
                out_ref[slice_no, k : k + 1, :] = row[slice_no : slice_no + 1]


def halves(x):
    high = x.astype(jnp.bfloat16)
    return high, (x - high.astype(jnp.float32)).astype(jnp.bfloat16)


def product(a, b, contract_b):
    dims = (((1,), (contract_b,)), ((), ()))
    dot = functools.partial(lax.dot_general, dimension_numbers=dims, preferred_element_type=jnp.float32)
    a_high, a_low = halves(a)
    b_high, b_low = halves(b)
    return dot(a_high, b_high) + (dot(a_high, b_low) + dot(a_low, b_high))


def mixed(w, u, rim, mix):
    before, after = LANES - 2, LANES
    rim_left = mix[4:5, before + 2 * LANES : before + 2 * LANES + 1] * rim[0] + mix[4:5, before : before + 1] * rim[1]
    rim_right = mix[4:5, after : after + 1] * rim[2] + mix[4:5, after + 2 * LANES : after + 2 * LANES + 1] * rim[3]
    end_left = jnp.sum(u * rim_left, axis=1, keepdims=True)
    end_right = jnp.sum(u * rim_right, axis=1, keepdims=True)
    count = w.shape[1]
    lane = lax.broadcasted_iota(jnp.int32, w.shape, 1)
    even = lane % 2 == 0
    partner = jnp.where(even, pltpu.roll(w, count - 1, 1), pltpu.roll(w, 1, 1))
    e = mix[0:1] * w + mix[1:2] * partner
    below = jnp.where(lane == 0, end_left, pltpu.roll(e, 1, 1))
    above = jnp.where(lane == count - 1, end_right, pltpu.roll(e, count - 1, 1))
    return mix[2:3] * e + mix[3:4] * jnp.where(even, below, above)


def joined(pieces):
    return jnp.concatenate(pieces, axis=1)


def in_rows(x, row):
    return [x[row : row + 1, k * LANES : (k + 1) * LANES] for k in range(x.shape[1] // LANES)]


def keep_rims(ref, rows):
    ref[...] = jnp.zeros(ref.shape, ref.dtype)
    for k, row in enumerate(rows):
        ref[k : k + 1, :] = row


def first_kernel(ids_ref, g_ref, mine_ref, other_ref, mix_ref, out_ref, rim_ref):
    core, row, z, high = ids_ref[0], ids_ref[1], ids_ref[2], ids_ref[3]
    peers = g_ref.shape[0] // 2
    width = mine_ref.shape[1]
    columns = peers * g_ref.shape[1]

    def of_core(k):
        return g_ref[pl.ds(k * peers, peers), :, 0:width].reshape(columns, width)

    w = product(of_core(core), mine_ref[...], 1) + product(of_core(1 - core), other_ref[...], 1)
    u = joined([of_core(0), of_core(1)])
    low, top = [], []
    for k in range(2):
        low.append(g_ref[k * peers + (row + peers - 1) % peers, :, width : width + LANES])
        top.append(g_ref[k * peers + (row + 1) % peers, :, width : width + LANES])
    rows = [
        joined([tile[2 * j + i : 2 * j + i + 1] for tile in tiles for i in range(2)])
        for tiles, start in ((low, 0), (top, 2))
        for j in (start, start + 1)
    ]
    keep_rims(rim_ref, rows)
    groups = out_ref.shape[0]
    out_ref[:, :, 0 : w.shape[1]] = mixed(w, u, rows, mix_ref[...]).reshape(groups, columns // groups, w.shape[1])

    upper = jnp.where(core == 1, mine_ref[:, width - LANES :], other_ref[:, width - LANES :]).T
    lower = jnp.where(core == 0, mine_ref[:, :LANES], other_ref[:, :LANES]).T
    tail = jnp.concatenate(in_rows(upper, LANES - 2) + in_rows(upper, LANES - 1), axis=0)
    head = jnp.concatenate(in_rows(lower, 0) + in_rows(lower, 1), axis=0)
    tail_to = (z + high) % groups
    head_to = (z + groups - 1 + high) % groups
    for p in range(groups):
        out_ref[p, 0:8, w.shape[1] :] = jnp.where(tail_to == p, tail, 0.0)
        out_ref[p, 8:16, w.shape[1] :] = jnp.where(head_to == p, head, 0.0)


def along_product(core, u, mine_ref, other_ref, w_ref):
    width = mine_ref.shape[1]
    w_ref[:, pl.ds(pl.multiple_of(core * width, width), width)] = product(u, mine_ref[...], 0)
    w_ref[:, pl.ds(pl.multiple_of((1 - core) * width, width), width)] = product(u, other_ref[...], 0)
    return w_ref[...]


def second_kernel(ids_ref, u_ref, ends_ref, mine_ref, other_ref, mix_ref, out_ref, rim_ref, w_ref):
    u = u_ref[...]
    w = along_product(ids_ref[0], u, mine_ref, other_ref, w_ref)
    rows = [joined([ends_ref[4 * j + k : 4 * j + k + 1, :] for k in range(4)]) for j in range(4)]
    keep_rims(rim_ref, rows)
    out_ref[...] = mixed(w, u, rows, mix_ref[...])


def third_kernel(ids_ref, u_ref, mine_ref, other_ref, rim_ref, mix_ref, out_ref):
    width = mine_ref.shape[1]
    core = ids_ref[0]
    u_mine = u_ref[:, pl.ds(pl.multiple_of(core * width, width), width)]
    u_other = u_ref[:, pl.ds(pl.multiple_of((1 - core) * width, width), width)]
    w = product(u_mine, mine_ref[...], 1) + product(u_other, other_ref[...], 1)
    rows = [rim_ref[k : k + 1, :] for k in range(4)]
    out_ref[...] = mixed(w, u_ref[...], rows, mix_ref[...])


def fourth_kernel(ids_ref, u_ref, mine_ref, other_ref, rim_ref, mix_ref, out_ref, w_ref):
    u = u_ref[...]
    w = along_product(ids_ref[0], u, mine_ref, other_ref, w_ref)
    rows = [rim_ref[k : k + 1, :] for k in range(4)]
    f = mixed(w, u, rows, mix_ref[...])
    width = out_ref.shape[2]
    peers = out_ref.shape[0] // 2
    for k in range(2):
        out_ref[k * peers : (k + 1) * peers] = f[:, k * width : (k + 1) * width].reshape(peers, 8, width)


def shards(propagator, slab, fields, phonon, couplings):
    block, width = propagator.shape
    count = 2 * width
    columns = slab.T
    half = columns.shape[0] // 2
    peers = lax.axis_size(ROW)
    groups = lax.axis_size("z")
    held = peers * half

    def full(*shape):
        return jax.ShapeDtypeStruct(shape, jnp.float32)

    mine = propagator
    other = swapped(propagator, "core")

    rims = jnp.concatenate([mine[-2:].reshape(4, LANES), mine[:2].reshape(4, LANES)])
    parts = jnp.stack([jnp.concatenate([columns[k * half : (k + 1) * half], rims], axis=1) for k in range(2)])
    parts = jnp.broadcast_to(parts[:, None], (2, peers, half, width + LANES))
    g = exchanged(parts.reshape(2 * peers, half, width + LANES), PAIRED_ROW)

    places = ("core", ROW, "z", "yhi")
    ids = jnp.stack([lax.axis_index(place) for place in places]).astype(jnp.int32)
    first = jnp.stack([lax.axis_index(ROW) * block, lax.axis_index(CUT) * count]).astype(jnp.int32)
    mix = call(
        mixing_kernel, "mixing", full(SLICES, 8, count), [SMEM, SMEM, VMEM, VMEM], size=4 * 10 * SITES
    )(first, couplings, phonon, fields)

    work = dict(flops=12 * held * block * count, size=8 * block * count)
    out, row_rim = call(
        first_kernel, "first", (full(groups, 2 * half, block + LANES), full(8, count)), [SMEM] + [VMEM] * 4, **work
    )(ids, g, mine, other, mix[0])
    share = exchanged(out, "z").sum(axis=0)
    across = swapped(share, "yhi")
    u = gathered(share[:, :block] + across[:, :block], "z")

    scratch = [pltpu.VMEM((held, count), jnp.float32)]
    w, cut_rim = call(
        second_kernel, "second", (full(held, count), full(8, block)), [SMEM] + [VMEM] * 5, scratch, **work
    )(ids, u, across[:, block:], mine, other, mix[1])
    u = gathered(summed(w, ROW), ROW)

    w = call(third_kernel, "third", full(held, block), [SMEM] + [VMEM] * 5, **work)(
        ids, u, mine, other, row_rim, mix[2]
    )
    share = summed(w, "z")
    u = gathered(share + swapped(share, "yhi"), "z")

    parts = call(
        fourth_kernel, "fourth", full(2 * peers, half, width), [SMEM] + [VMEM] * 5, scratch, **work
    )(ids, u, mine, other, cut_rim, mix[3])
    out = exchanged(parts, PAIRED_ROW).reshape(2, peers, half, width).sum(axis=1)
    return out.reshape(2 * half, width).T


def solution(mesh):
    devices = mesh.devices.reshape(8, 2, 2, 4, 4)
    fine = Mesh(devices, ("z", "yhi", "core", "x", "ylo"))
    cuts = ("z", "yhi", "core")
    in_specs = (P(ROW, cuts), P(cuts, ROW), P(), P(), P())
    return jax.shard_map(shards, mesh=fine, in_specs=in_specs, out_specs=P(cuts, ROW), check_vma=False)
```

```python
import functools

import jax
import jax.numpy as jnp
from jax import lax
from jax.experimental import pallas as pl
from jax.experimental.pallas import tpu as pltpu
from jax.sharding import Mesh, PartitionSpec as P

SITES = 8192
SLICES = 4
LEVELS = 16
LANES = 128

hs_strength = 0.3

ROW = ("x", "ylo")
CUT = ("z", "yhi")
PAIRED_ROW = ("core", "x", "ylo")

VMEM = pl.BlockSpec(memory_space=pltpu.VMEM)
SMEM = pl.BlockSpec(memory_space=pltpu.SMEM)


def swapped(x, axis):
    return lax.ppermute(x, axis, [(0, 1), (1, 0)])


def exchanged(parts, axes):
    return lax.all_to_all(parts, axes, 0, 0, tiled=True)


def gathered(x, axes):
    count = lax.axis_size(axes)
    parts = exchanged(jnp.broadcast_to(x[None], (count, *x.shape)), axes)
    return parts.reshape(count * x.shape[0], x.shape[1])


def summed(x, axes):
    count = lax.axis_size(axes)
    return exchanged(x.reshape(count, x.shape[0] // count, x.shape[1]), axes).sum(axis=0)


def call(kernel, name, out_shape, in_specs, scratch=(), flops=0, size=0):
    return pl.pallas_call(
        kernel,
        out_shape=out_shape,
        in_specs=in_specs,
        out_specs=jax.tree.map(lambda _: VMEM, out_shape),
        scratch_shapes=list(scratch),
        compiler_params=pltpu.CompilerParams(vmem_limit_bytes=24 * 1024 * 1024),
        cost_estimate=pl.CostEstimate(flops=flops, bytes_accessed=size, transcendentals=0),
        name=name,
    )


def mixing_kernel(first_ref, couplings_ref, phonon_ref, fields_ref, out_ref):
    count = out_ref.shape[2]
    for turn in range(2):
        first = first_ref[turn]
        at_before = pl.ds(pl.multiple_of((first + (SITES - LANES)) % SITES, LANES), LANES)
        at_block = pl.ds(pl.multiple_of(first, LANES), count)
        at_after = pl.ds(pl.multiple_of((first + count) % SITES, LANES), LANES)
        level = jnp.concatenate([phonon_ref[:, at_before], phonon_ref[:, at_block], phonon_ref[:, at_after]], axis=1)
        rate = jnp.zeros(level.shape, jnp.float32)
        for k in range(LEVELS):
            rate = jnp.where(level == k, couplings_ref[k], rate)
        grown, shrunk = jnp.exp(rate), jnp.exp(-rate)
        cosh, sinh = 0.5 * (grown + shrunk), 0.5 * (grown - shrunk)
        cosh_left, sinh_left = pltpu.roll(cosh, 1, 1), pltpu.roll(sinh, 1, 1)
        even = lax.broadcasted_iota(jnp.int32, rate.shape, 1) % 2 == 0
        inside = slice(LANES, LANES + count)
        sign = (2 * fields_ref[:, at_block] - 1).astype(jnp.float32)
        scale = jnp.exp(hs_strength * sign)
        rows = [
            jnp.where(even, cosh, cosh_left)[:, inside],
            jnp.where(even, sinh, sinh_left)[:, inside],
            scale * jnp.where(even, cosh_left, cosh)[:, inside],
            scale * jnp.where(even, sinh_left, sinh)[:, inside],
            jnp.concatenate(
                [cosh[:, :LANES], cosh[:, LANES + count :], sinh[:, :LANES], sinh[:, LANES + count :]], axis=1
            ),
        ]
        for slice_no in range(turn, SLICES, 2):
            for k, row in enumerate(rows):
                out_ref[slice_no, k : k + 1, :] = row[slice_no : slice_no + 1]


def halves(x):
    high = x.astype(jnp.bfloat16)
    return high, (x - high.astype(jnp.float32)).astype(jnp.bfloat16)


def split_kernel(mine_ref, other_ref, *out_refs):
    for k, ref in enumerate((mine_ref, other_ref)):
        out_refs[2 * k][...], out_refs[2 * k + 1][...] = halves(ref[...])


def product(a, b_high_ref, b_low_ref, contract_b):
    dims = (((1,), (contract_b,)), ((), ()))
    dot = functools.partial(lax.dot_general, dimension_numbers=dims, preferred_element_type=jnp.float32)
    a_high, a_low = halves(a)
    both = dot(jnp.concatenate([a_high, a_low], axis=0), b_high_ref[...])
    count = a.shape[0]
    return both[:count] + (both[count:] + dot(a_high, b_low_ref[...]))


def mixed(w, u, rim, mix):
    before, after = LANES - 2, LANES
    rim_left = mix[4:5, before + 2 * LANES : before + 2 * LANES + 1] * rim[0] + mix[4:5, before : before + 1] * rim[1]
    rim_right = mix[4:5, after : after + 1] * rim[2] + mix[4:5, after + 2 * LANES : after + 2 * LANES + 1] * rim[3]
    end_left = jnp.sum(u * rim_left, axis=1, keepdims=True)
    end_right = jnp.sum(u * rim_right, axis=1, keepdims=True)
    count = w.shape[1]
    lane = lax.broadcasted_iota(jnp.int32, w.shape, 1)
    even = lane % 2 == 0
    partner = jnp.where(even, pltpu.roll(w, count - 1, 1), pltpu.roll(w, 1, 1))
    e = mix[0:1] * w + mix[1:2] * partner
    below = jnp.where(lane == 0, end_left, pltpu.roll(e, 1, 1))
    above = jnp.where(lane == count - 1, end_right, pltpu.roll(e, count - 1, 1))
    return mix[2:3] * e + mix[3:4] * jnp.where(even, below, above)


def joined(pieces):
    return jnp.concatenate(pieces, axis=1)


def in_rows(x, row):
    return [x[row : row + 1, k * LANES : (k + 1) * LANES] for k in range(x.shape[1] // LANES)]


def keep_rims(ref, rows):
    ref[...] = jnp.zeros(ref.shape, ref.dtype)
    for k, row in enumerate(rows):
        ref[k : k + 1, :] = row


def first_kernel(ids_ref, g_ref, mine_ref, other_ref, mh_ref, ml_ref, oh_ref, ol_ref, mix_ref, out_ref, rim_ref):
    core, row, z, high = ids_ref[0], ids_ref[1], ids_ref[2], ids_ref[3]
    peers = g_ref.shape[0] // 2
    width = mine_ref.shape[1]
    columns = peers * g_ref.shape[1]

    def of_core(k):
        return g_ref[pl.ds(k * peers, peers), :, 0:width].reshape(columns, width)

    w = product(of_core(core), mh_ref, ml_ref, 1) + product(of_core(1 - core), oh_ref, ol_ref, 1)
    u = joined([of_core(0), of_core(1)])
    low, top = [], []
    for k in range(2):
        low.append(g_ref[k * peers + (row + peers - 1) % peers, :, width : width + LANES])
        top.append(g_ref[k * peers + (row + 1) % peers, :, width : width + LANES])
    rows = [
        joined([tile[2 * j + i : 2 * j + i + 1] for tile in tiles for i in range(2)])
        for tiles, start in ((low, 0), (top, 2))
        for j in (start, start + 1)
    ]
    keep_rims(rim_ref, rows)
    groups = out_ref.shape[0]
    out_ref[:, :, 0 : w.shape[1]] = mixed(w, u, rows, mix_ref[0]).reshape(groups, columns // groups, w.shape[1])

    upper = jnp.where(core == 1, mine_ref[:, width - LANES :], other_ref[:, width - LANES :]).T
    lower = jnp.where(core == 0, mine_ref[:, :LANES], other_ref[:, :LANES]).T
    tail = jnp.concatenate(in_rows(upper, LANES - 2) + in_rows(upper, LANES - 1), axis=0)
    head = jnp.concatenate(in_rows(lower, 0) + in_rows(lower, 1), axis=0)
    tail_to = (z + high) % groups
    head_to = (z + groups - 1 + high) % groups
    for p in range(groups):
        out_ref[p, 0:8, w.shape[1] :] = jnp.where(tail_to == p, tail, 0.0)
        out_ref[p, 8:16, w.shape[1] :] = jnp.where(head_to == p, head, 0.0)


def along_product(core, u, mh_ref, ml_ref, oh_ref, ol_ref, w_ref):
    width = mh_ref.shape[1]
    w_ref[:, pl.ds(pl.multiple_of(core * width, width), width)] = product(u, mh_ref, ml_ref, 0)
    w_ref[:, pl.ds(pl.multiple_of((1 - core) * width, width), width)] = product(u, oh_ref, ol_ref, 0)
    return w_ref[...]


def second_kernel(ids_ref, u_ref, ends_ref, mh_ref, ml_ref, oh_ref, ol_ref, mix_ref, out_ref, rim_ref, w_ref):
    u = u_ref[...]
    w = along_product(ids_ref[0], u, mh_ref, ml_ref, oh_ref, ol_ref, w_ref)
    at = u.shape[1]
    rows = [joined([ends_ref[4 * j + k : 4 * j + k + 1, at : at + LANES] for k in range(4)]) for j in range(4)]
    keep_rims(rim_ref, rows)
    out_ref[...] = mixed(w, u, rows, mix_ref[1])


def third_kernel(ids_ref, u_ref, mh_ref, ml_ref, oh_ref, ol_ref, rim_ref, mix_ref, out_ref):
    width = mh_ref.shape[1]
    core = ids_ref[0]
    u_mine = u_ref[:, pl.ds(pl.multiple_of(core * width, width), width)]
    u_other = u_ref[:, pl.ds(pl.multiple_of((1 - core) * width, width), width)]
    w = product(u_mine, mh_ref, ml_ref, 1) + product(u_other, oh_ref, ol_ref, 1)
    rows = [rim_ref[k : k + 1, :] for k in range(4)]
    out_ref[...] = mixed(w, u_ref[...], rows, mix_ref[2])


def fourth_kernel(ids_ref, u_ref, mh_ref, ml_ref, oh_ref, ol_ref, rim_ref, mix_ref, out_ref, w_ref):
    u = u_ref[...]
    w = along_product(ids_ref[0], u, mh_ref, ml_ref, oh_ref, ol_ref, w_ref)
    rows = [rim_ref[k : k + 1, :] for k in range(4)]
    f = mixed(w, u, rows, mix_ref[3])
    width = out_ref.shape[2]
    peers = out_ref.shape[0] // 2
    for k in range(2):
        out_ref[k * peers : (k + 1) * peers] = f[:, k * width : (k + 1) * width].reshape(peers, 8, width)


def shards(propagator, slab, fields, phonon, couplings):
    block, width = propagator.shape
    count = 2 * width
    columns = slab.T
    half = columns.shape[0] // 2
    peers = lax.axis_size(ROW)
    groups = lax.axis_size("z")
    held = peers * half

    def full(*shape):
        return jax.ShapeDtypeStruct(shape, jnp.float32)

    mine = propagator
    other = swapped(propagator, "core")

    rims = jnp.concatenate([mine[-2:].reshape(4, LANES), mine[:2].reshape(4, LANES)])
    parts = jnp.stack([jnp.concatenate([columns[k * half : (k + 1) * half], rims], axis=1) for k in range(2)])
    parts = jnp.broadcast_to(parts[:, None], (2, peers, half, width + LANES))
    g = exchanged(parts.reshape(2 * peers, half, width + LANES), PAIRED_ROW)

    places = ("core", ROW, "z", "yhi")
    ids = jnp.stack([lax.axis_index(place) for place in places]).astype(jnp.int32)
    first = jnp.stack([lax.axis_index(ROW) * block, lax.axis_index(CUT) * count]).astype(jnp.int32)
    mix = call(
        mixing_kernel, "mixing", full(SLICES, 8, count), [SMEM, SMEM, VMEM, VMEM], size=4 * 10 * SITES
    )(first, couplings, phonon, fields)

    split = jax.ShapeDtypeStruct((block, width), jnp.bfloat16)
    pieces = call(split_kernel, "split", (split,) * 4, [VMEM, VMEM], size=16 * block * width)(mine, other)

    work = dict(flops=12 * held * block * count, size=8 * block * count)
    out, row_rim = call(
        first_kernel, "first", (full(groups, 2 * half, block + LANES), full(8, count)), [SMEM] + [VMEM] * 8, **work
    )(ids, g, mine, other, *pieces, mix)
    share = exchanged(out, "z").sum(axis=0)
    across = swapped(share, "yhi")
    u = gathered(share[:, :block] + across[:, :block], "z")

    scratch = [pltpu.VMEM((held, count), jnp.float32)]
    w, cut_rim = call(
        second_kernel, "second", (full(held, count), full(8, block)), [SMEM] + [VMEM] * 7, scratch, **work
    )(ids, u, across, *pieces, mix)
    u = gathered(summed(w, ROW), ROW)

    w = call(third_kernel, "third", full(held, block), [SMEM] + [VMEM] * 7, **work)(
        ids, u, *pieces, row_rim, mix
    )
    share = summed(w, "z")
    u = gathered(share + swapped(share, "yhi"), "z")

    parts = call(
        fourth_kernel, "fourth", full(2 * peers, half, width), [SMEM] + [VMEM] * 7, scratch, **work
    )(ids, u, *pieces, cut_rim, mix)
    out = exchanged(parts, PAIRED_ROW).reshape(2, peers, half, width).sum(axis=1)
    return out.reshape(2 * half, width).T


def solution(mesh):
    devices = mesh.devices.reshape(8, 2, 2, 4, 4)
    fine = Mesh(devices, ("z", "yhi", "core", "x", "ylo"))
    cuts = ("z", "yhi", "core")
    in_specs = (P(ROW, cuts), P(cuts, ROW), P(), P(), P())
    return jax.shard_map(shards, mesh=fine, in_specs=in_specs, out_specs=P(cuts, ROW), check_vma=False)
```

```python
import functools

import jax
import jax.numpy as jnp
from jax import lax
from jax.experimental import pallas as pl
from jax.experimental.pallas import tpu as pltpu
from jax.sharding import Mesh, PartitionSpec as P

SITES = 8192
SLICES = 4
LEVELS = 16
LANES = 128

hs_strength = 0.3

ROW = ("x", "ylo")
CUT = ("z", "yhi")
PAIRED_ROW = ("core", "x", "ylo")

VMEM = pl.BlockSpec(memory_space=pltpu.VMEM)
SMEM = pl.BlockSpec(memory_space=pltpu.SMEM)


def swapped(x, axis):
    return lax.ppermute(x, axis, [(0, 1), (1, 0)])


def exchanged(parts, axes):
    return lax.all_to_all(parts, axes, 0, 0, tiled=True)


def from_all(x, axes):
    return exchanged(jnp.broadcast_to(x[None], (lax.axis_size(axes), *x.shape)), axes)


def gathered(x, axes):
    return from_all(x, axes).reshape(-1, x.shape[1])


def summed(x, axes):
    count = lax.axis_size(axes)
    return exchanged(x.reshape(count, x.shape[0] // count, x.shape[1]), axes).sum(axis=0)


def call(kernel, name, out_shape, in_specs, scratch=(), flops=0, size=0):
    return pl.pallas_call(
        kernel,
        out_shape=out_shape,
        in_specs=in_specs,
        out_specs=jax.tree.map(lambda _: VMEM, out_shape),
        scratch_shapes=list(scratch),
        compiler_params=pltpu.CompilerParams(vmem_limit_bytes=24 * 1024 * 1024),
        cost_estimate=pl.CostEstimate(flops=flops, bytes_accessed=size, transcendentals=0),
        name=name,
    )


def mixing_kernel(first_ref, couplings_ref, phonon_ref, fields_ref, out_ref):
    count = out_ref.shape[2]
    for turn in range(2):
        first = first_ref[turn]
        at_before = pl.ds(pl.multiple_of((first + (SITES - LANES)) % SITES, LANES), LANES)
        at_block = pl.ds(pl.multiple_of(first, LANES), count)
        at_after = pl.ds(pl.multiple_of((first + count) % SITES, LANES), LANES)
        level = jnp.concatenate([phonon_ref[:, at_before], phonon_ref[:, at_block], phonon_ref[:, at_after]], axis=1)
        rate = jnp.zeros(level.shape, jnp.float32)
        for k in range(LEVELS):
            rate = jnp.where(level == k, couplings_ref[k], rate)
        grown, shrunk = jnp.exp(rate), jnp.exp(-rate)
        cosh, sinh = 0.5 * (grown + shrunk), 0.5 * (grown - shrunk)
        cosh_left, sinh_left = pltpu.roll(cosh, 1, 1), pltpu.roll(sinh, 1, 1)
        even = lax.broadcasted_iota(jnp.int32, rate.shape, 1) % 2 == 0
        inside = slice(LANES, LANES + count)
        sign = (2 * fields_ref[:, at_block] - 1).astype(jnp.float32)
        scale = jnp.exp(hs_strength * sign)
        rows = [
            jnp.where(even, cosh, cosh_left)[:, inside],
            jnp.where(even, sinh, sinh_left)[:, inside],
            scale * jnp.where(even, cosh_left, cosh)[:, inside],
            scale * jnp.where(even, sinh_left, sinh)[:, inside],
            jnp.concatenate(
                [cosh[:, :LANES], cosh[:, LANES + count :], sinh[:, :LANES], sinh[:, LANES + count :]], axis=1
            ),
        ]
        for slice_no in range(turn, SLICES, 2):
            for k, row in enumerate(rows):
                out_ref[slice_no, k : k + 1, :] = row[slice_no : slice_no + 1]


def halves(x):
    high = x.astype(jnp.bfloat16)
    return high, (x - high.astype(jnp.float32)).astype(jnp.bfloat16)


def split_kernel(mine_ref, other_ref, *out_refs):
    for k, ref in enumerate((mine_ref, other_ref)):
        out_refs[2 * k][...], out_refs[2 * k + 1][...] = halves(ref[...])


def product(a, b_high_ref, b_low_ref, contract_b):
    dims = (((1,), (contract_b,)), ((), ()))
    dot = functools.partial(lax.dot_general, dimension_numbers=dims, preferred_element_type=jnp.float32)
    a_high, a_low = halves(a)
    both = dot(jnp.concatenate([a_high, a_low], axis=0), b_high_ref[...])
    count = a.shape[0]
    return both[:count] + (both[count:] + dot(a_high, b_low_ref[...]))


def mixed(w, u, rim, mix):
    before, after = LANES - 2, LANES
    rim_left = mix[4:5, before + 2 * LANES : before + 2 * LANES + 1] * rim[0] + mix[4:5, before : before + 1] * rim[1]
    rim_right = mix[4:5, after : after + 1] * rim[2] + mix[4:5, after + 2 * LANES : after + 2 * LANES + 1] * rim[3]
    end_left = jnp.sum(u * rim_left, axis=1, keepdims=True)
    end_right = jnp.sum(u * rim_right, axis=1, keepdims=True)
    count = w.shape[1]
    lane = lax.broadcasted_iota(jnp.int32, w.shape, 1)
    even = lane % 2 == 0
    partner = jnp.where(even, pltpu.roll(w, count - 1, 1), pltpu.roll(w, 1, 1))
    e = mix[0:1] * w + mix[1:2] * partner
    below = jnp.where(lane == 0, end_left, pltpu.roll(e, 1, 1))
    above = jnp.where(lane == count - 1, end_right, pltpu.roll(e, count - 1, 1))
    return mix[2:3] * e + mix[3:4] * jnp.where(even, below, above)


def joined(pieces):
    return jnp.concatenate(pieces, axis=1)


def in_rows(x, row):
    return [x[row : row + 1, k * LANES : (k + 1) * LANES] for k in range(x.shape[1] // LANES)]


def keep_rims(ref, rows):
    ref[...] = jnp.zeros(ref.shape, ref.dtype)
    for k, row in enumerate(rows):
        ref[k : k + 1, :] = row


def pack_kernel(columns_ref, low_ref, high_ref, out_ref):
    ends = in_rows(high_ref, 6) + in_rows(high_ref, 7) + in_rows(low_ref, 0) + in_rows(low_ref, 1)
    rims = jnp.concatenate(ends, axis=0)
    peers, half = out_ref.shape[0] // 2, out_ref.shape[1]
    for k in range(2):
        part = joined([columns_ref[k * half : (k + 1) * half, :], rims])
        out_ref[k * peers : (k + 1) * peers] = jnp.broadcast_to(part[None], (peers, *part.shape))


def first_kernel(ids_ref, g_ref, mine_ref, other_ref, mh_ref, ml_ref, oh_ref, ol_ref, mix_ref, out_ref, rim_ref):
    core, row, z, high = ids_ref[0], ids_ref[1], ids_ref[2], ids_ref[3]
    peers = g_ref.shape[0] // 2
    width = mine_ref.shape[1]
    columns = peers * g_ref.shape[1]

    def of_core(k):
        return g_ref[pl.ds(k * peers, peers), :, 0:width].reshape(columns, width)

    w = product(of_core(core), mh_ref, ml_ref, 1) + product(of_core(1 - core), oh_ref, ol_ref, 1)
    u = joined([of_core(0), of_core(1)])
    low, top = [], []
    for k in range(2):
        low.append(g_ref[k * peers + (row + peers - 1) % peers, :, width : width + LANES])
        top.append(g_ref[k * peers + (row + 1) % peers, :, width : width + LANES])
    rows = [
        joined([tile[2 * j + i : 2 * j + i + 1] for tile in tiles for i in range(2)])
        for tiles, start in ((low, 0), (top, 2))
        for j in (start, start + 1)
    ]
    keep_rims(rim_ref, rows)
    groups = out_ref.shape[0]
    out_ref[:, :, 0 : w.shape[1]] = mixed(w, u, rows, mix_ref[0]).reshape(groups, columns // groups, w.shape[1])

    upper = jnp.where(core == 1, mine_ref[:, width - LANES :], other_ref[:, width - LANES :]).T
    lower = jnp.where(core == 0, mine_ref[:, :LANES], other_ref[:, :LANES]).T
    tail = jnp.concatenate(in_rows(upper, LANES - 2) + in_rows(upper, LANES - 1), axis=0)
    head = jnp.concatenate(in_rows(lower, 0) + in_rows(lower, 1), axis=0)
    tail_to = (z + high) % groups
    head_to = (z + groups - 1 + high) % groups
    for p in range(groups):
        out_ref[p, 0:8, w.shape[1] :] = jnp.where(tail_to == p, tail, 0.0)
        out_ref[p, 8:16, w.shape[1] :] = jnp.where(head_to == p, head, 0.0)


def along_product(core, u, mh_ref, ml_ref, oh_ref, ol_ref, w_ref):
    width = mh_ref.shape[1]
    w_ref[:, pl.ds(pl.multiple_of(core * width, width), width)] = product(u, mh_ref, ml_ref, 0)
    w_ref[:, pl.ds(pl.multiple_of((1 - core) * width, width), width)] = product(u, oh_ref, ol_ref, 0)
    return w_ref[...]


def second_kernel(ids_ref, u_ref, ends_ref, mh_ref, ml_ref, oh_ref, ol_ref, mix_ref, out_ref, rim_ref, w_ref):
    u = u_ref[...]
    w = along_product(ids_ref[0], u, mh_ref, ml_ref, oh_ref, ol_ref, w_ref)
    ends = ends_ref[1 - ids_ref[3], :, u.shape[1] :]
    rows = [joined([ends[4 * j + k : 4 * j + k + 1] for k in range(4)]) for j in range(4)]
    keep_rims(rim_ref, rows)
    out_ref[...] = mixed(w, u, rows, mix_ref[1])


def third_kernel(ids_ref, u_ref, mh_ref, ml_ref, oh_ref, ol_ref, rim_ref, mix_ref, out_ref):
    width = mh_ref.shape[1]
    core = ids_ref[0]
    u_mine = u_ref[:, pl.ds(pl.multiple_of(core * width, width), width)]
    u_other = u_ref[:, pl.ds(pl.multiple_of((1 - core) * width, width), width)]
    w = product(u_mine, mh_ref, ml_ref, 1) + product(u_other, oh_ref, ol_ref, 1)
    rows = [rim_ref[k : k + 1, :] for k in range(4)]
    out_ref[...] = mixed(w, u_ref[...], rows, mix_ref[2])


def fourth_kernel(ids_ref, u_ref, mh_ref, ml_ref, oh_ref, ol_ref, rim_ref, mix_ref, out_ref, w_ref):
    u = u_ref[...]
    w = along_product(ids_ref[0], u, mh_ref, ml_ref, oh_ref, ol_ref, w_ref)
    rows = [rim_ref[k : k + 1, :] for k in range(4)]
    f = mixed(w, u, rows, mix_ref[3])
    width = out_ref.shape[2]
    peers = out_ref.shape[0] // 2
    for k in range(2):
        out_ref[k * peers : (k + 1) * peers] = f[:, k * width : (k + 1) * width].reshape(peers, 8, width)


def shards(propagator, slab, fields, phonon, couplings):
    block, width = propagator.shape
    count = 2 * width
    columns = slab.T
    half = columns.shape[0] // 2
    peers = lax.axis_size(ROW)
    groups = lax.axis_size("z")
    held = peers * half

    def full(*shape):
        return jax.ShapeDtypeStruct(shape, jnp.float32)

    mine = propagator
    other = swapped(propagator, "core")

    parts = full(2 * peers, half, width + LANES)
    parts = pl.pallas_call(
        pack_kernel,
        grid=(1,),
        out_shape=parts,
        in_specs=[
            pl.BlockSpec(columns.shape, lambda i: (0, 0)),
            pl.BlockSpec((8, width), lambda i: (0, 0)),
            pl.BlockSpec((8, width), lambda i: (block // 8 - 1, 0)),
        ],
        out_specs=pl.BlockSpec(parts.shape, lambda i: (0, 0, 0)),
        compiler_params=pltpu.CompilerParams(vmem_limit_bytes=60 * 1024 * 1024),
        name="pack",
    )(columns, mine, mine)
    g = exchanged(parts, PAIRED_ROW)

    places = ("core", ROW, "z", "yhi")
    ids = jnp.stack([lax.axis_index(place) for place in places]).astype(jnp.int32)
    first = jnp.stack([lax.axis_index(ROW) * block, lax.axis_index(CUT) * count]).astype(jnp.int32)
    mix = call(
        mixing_kernel, "mixing", full(SLICES, 8, count), [SMEM, SMEM, VMEM, VMEM], size=4 * 10 * SITES
    )(first, couplings, phonon, fields)

    split = jax.ShapeDtypeStruct((block, width), jnp.bfloat16)
    pieces = call(split_kernel, "split", (split,) * 4, [VMEM, VMEM], size=16 * block * width)(mine, other)

    work = dict(flops=12 * held * block * count, size=8 * block * count)
    out, row_rim = call(
        first_kernel, "first", (full(groups, 2 * half, block + LANES), full(8, count)), [SMEM] + [VMEM] * 8, **work
    )(ids, g, mine, other, *pieces, mix)
    share = exchanged(out, "z").sum(axis=0)
    both = from_all(share, "yhi")
    u = gathered(both[:, :, :block].sum(axis=0), "z")

    scratch = [pltpu.VMEM((held, count), jnp.float32)]
    w, cut_rim = call(
        second_kernel, "second", (full(held, count), full(8, block)), [SMEM] + [VMEM] * 7, scratch, **work
    )(ids, u, both, *pieces, mix)
    u = gathered(summed(w, ROW), ROW)

    w = call(third_kernel, "third", full(held, block), [SMEM] + [VMEM] * 7, **work)(
        ids, u, *pieces, row_rim, mix
    )
    share = summed(w, "z")
    u = gathered(from_all(share, "yhi").sum(axis=0), "z")

    parts = call(
        fourth_kernel, "fourth", full(2 * peers, half, width), [SMEM] + [VMEM] * 7, scratch, **work
    )(ids, u, *pieces, cut_rim, mix)
    out = exchanged(parts, PAIRED_ROW).reshape(2, peers, half, width).sum(axis=1)
    return out.reshape(2 * half, width).T


def solution(mesh):
    devices = mesh.devices.reshape(8, 2, 2, 4, 4)
    fine = Mesh(devices, ("z", "yhi", "core", "x", "ylo"))
    cuts = ("z", "yhi", "core")
    in_specs = (P(ROW, cuts), P(cuts, ROW), P(), P(), P())
    return jax.shard_map(shards, mesh=fine, in_specs=in_specs, out_specs=P(cuts, ROW), check_vma=False)
```

```python
import functools

import jax
import jax.numpy as jnp
from jax import lax
from jax.experimental import pallas as pl
from jax.experimental.pallas import tpu as pltpu
from jax.sharding import Mesh, PartitionSpec as P

SITES = 8192
SLICES = 4
LEVELS = 16
LANES = 128

hs_strength = 0.3

ROW = ("x", "ylo")
CUT = ("z", "yhi")
PAIRED_ROW = ("core", "x", "ylo")

VMEM = pl.BlockSpec(memory_space=pltpu.VMEM)


def swapped(x, axis):
    return lax.ppermute(x, axis, [(0, 1), (1, 0)])


def exchanged(parts, axes):
    return lax.all_to_all(parts, axes, 0, 0, tiled=True)


def gathered(x, axes):
    count = lax.axis_size(axes)
    parts = exchanged(jnp.broadcast_to(x[None], (count, *x.shape)), axes)
    return parts.reshape(count * x.shape[0], x.shape[1])


def summed(x, axes):
    count = lax.axis_size(axes)
    return exchanged(x.reshape(count, x.shape[0] // count, x.shape[1]), axes).sum(axis=0)


def call(kernel, name, out_shape, in_specs, scratch=(), flops=0, size=0):
    return pl.pallas_call(
        kernel,
        out_shape=out_shape,
        in_specs=in_specs,
        out_specs=jax.tree.map(lambda _: VMEM, out_shape),
        scratch_shapes=list(scratch),
        compiler_params=pltpu.CompilerParams(vmem_limit_bytes=24 * 1024 * 1024),
        cost_estimate=pl.CostEstimate(flops=flops, bytes_accessed=size, transcendentals=0),
        name=name,
    )


def place(axes):
    at = 0
    for axis in axes:
        at = at * lax.axis_size(axis) + lax.axis_index(axis)
    return at


def mixing_kernel(block, couplings_ref, phonon_ref, fields_ref, out_ref):
    count = out_ref.shape[2]
    for turn in range(2):
        first = place(ROW) * block if turn == 0 else place(CUT) * count
        at_before = pl.ds(pl.multiple_of((first + (SITES - LANES)) % SITES, LANES), LANES)
        at_block = pl.ds(pl.multiple_of(first, LANES), count)
        at_after = pl.ds(pl.multiple_of((first + count) % SITES, LANES), LANES)
        level = jnp.concatenate([phonon_ref[:, at_before], phonon_ref[:, at_block], phonon_ref[:, at_after]], axis=1)
        rate = jnp.zeros(level.shape, jnp.float32)
        for k in range(LEVELS):
            rate = jnp.where(level == k, couplings_ref[0:1, k : k + 1], rate)
        grown, shrunk = jnp.exp(rate), jnp.exp(-rate)
        cosh, sinh = 0.5 * (grown + shrunk), 0.5 * (grown - shrunk)
        cosh_left, sinh_left = pltpu.roll(cosh, 1, 1), pltpu.roll(sinh, 1, 1)
        even = lax.broadcasted_iota(jnp.int32, rate.shape, 1) % 2 == 0
        inside = slice(LANES, LANES + count)
        sign = (2 * fields_ref[:, at_block] - 1).astype(jnp.float32)
        scale = jnp.exp(hs_strength * sign)
        rows = [
            jnp.where(even, cosh, cosh_left)[:, inside],
            jnp.where(even, sinh, sinh_left)[:, inside],
            scale * jnp.where(even, cosh_left, cosh)[:, inside],
            scale * jnp.where(even, sinh_left, sinh)[:, inside],
            jnp.concatenate(
                [cosh[:, :LANES], cosh[:, LANES + count :], sinh[:, :LANES], sinh[:, LANES + count :]], axis=1
            ),
        ]
        for slice_no in range(turn, SLICES, 2):
            for k, row in enumerate(rows):
                out_ref[slice_no, k : k + 1, :] = row[slice_no : slice_no + 1]


def halves(x):
    high = x.astype(jnp.bfloat16)
    return high, (x - high.astype(jnp.float32)).astype(jnp.bfloat16)


def split_kernel(mine_ref, other_ref, *out_refs):
    for k, ref in enumerate((mine_ref, other_ref)):
        out_refs[2 * k][...], out_refs[2 * k + 1][...] = halves(ref[...])


def product(a, b_high_ref, b_low_ref, contract_b):
    dims = (((1,), (contract_b,)), ((), ()))
    dot = functools.partial(lax.dot_general, dimension_numbers=dims, preferred_element_type=jnp.float32)
    a_high, a_low = halves(a)
    both = dot(jnp.concatenate([a_high, a_low], axis=0), b_high_ref[...])
    count = a.shape[0]
    return both[:count] + (both[count:] + dot(a_high, b_low_ref[...]))


def mixed(w, u, rim, mix):
    before, after = LANES - 2, LANES
    rim_left = mix[4:5, before + 2 * LANES : before + 2 * LANES + 1] * rim[0] + mix[4:5, before : before + 1] * rim[1]
    rim_right = mix[4:5, after : after + 1] * rim[2] + mix[4:5, after + 2 * LANES : after + 2 * LANES + 1] * rim[3]
    end_left = jnp.sum(u * rim_left, axis=1, keepdims=True)
    end_right = jnp.sum(u * rim_right, axis=1, keepdims=True)
    count = w.shape[1]
    lane = lax.broadcasted_iota(jnp.int32, w.shape, 1)
    even = lane % 2 == 0
    partner = jnp.where(even, pltpu.roll(w, count - 1, 1), pltpu.roll(w, 1, 1))
    e = mix[0:1] * w + mix[1:2] * partner
    below = jnp.where(lane == 0, end_left, pltpu.roll(e, 1, 1))
    above = jnp.where(lane == count - 1, end_right, pltpu.roll(e, count - 1, 1))
    return mix[2:3] * e + mix[3:4] * jnp.where(even, below, above)


def joined(pieces):
    return jnp.concatenate(pieces, axis=1)


def in_rows(x, row):
    return [x[row : row + 1, k * LANES : (k + 1) * LANES] for k in range(x.shape[1] // LANES)]


def keep_rims(ref, rows):
    ref[...] = jnp.zeros(ref.shape, ref.dtype)
    for k, row in enumerate(rows):
        ref[k : k + 1, :] = row


def first_kernel(g_ref, mine_ref, other_ref, mh_ref, ml_ref, oh_ref, ol_ref, mix_ref, out_ref, rim_ref):
    core, row, z, high = lax.axis_index("core"), place(ROW), lax.axis_index("z"), lax.axis_index("yhi")
    peers = g_ref.shape[0] // 2
    width = mine_ref.shape[1]
    columns = peers * g_ref.shape[1]

    def of_core(k):
        return g_ref[pl.ds(k * peers, peers), :, 0:width].reshape(columns, width)

    w = product(of_core(core), mh_ref, ml_ref, 1) + product(of_core(1 - core), oh_ref, ol_ref, 1)
    u = joined([of_core(0), of_core(1)])
    low, top = [], []
    for k in range(2):
        low.append(g_ref[k * peers + (row + peers - 1) % peers, :, width : width + LANES])
        top.append(g_ref[k * peers + (row + 1) % peers, :, width : width + LANES])
    rows = [
        joined([tile[2 * j + i : 2 * j + i + 1] for tile in tiles for i in range(2)])
        for tiles, start in ((low, 0), (top, 2))
        for j in (start, start + 1)
    ]
    keep_rims(rim_ref, rows)
    groups = out_ref.shape[0]
    out_ref[:, :, 0 : w.shape[1]] = mixed(w, u, rows, mix_ref[0]).reshape(groups, columns // groups, w.shape[1])

    upper = jnp.where(core == 1, mine_ref[:, width - LANES :], other_ref[:, width - LANES :]).T
    lower = jnp.where(core == 0, mine_ref[:, :LANES], other_ref[:, :LANES]).T
    tail = jnp.concatenate(in_rows(upper, LANES - 2) + in_rows(upper, LANES - 1), axis=0)
    head = jnp.concatenate(in_rows(lower, 0) + in_rows(lower, 1), axis=0)
    tail_to = (z + high) % groups
    head_to = (z + groups - 1 + high) % groups
    for p in range(groups):
        out_ref[p, 0:8, w.shape[1] :] = jnp.where(tail_to == p, tail, 0.0)
        out_ref[p, 8:16, w.shape[1] :] = jnp.where(head_to == p, head, 0.0)


def along_product(core, u, mh_ref, ml_ref, oh_ref, ol_ref, w_ref):
    width = mh_ref.shape[1]
    w_ref[:, pl.ds(pl.multiple_of(core * width, width), width)] = product(u, mh_ref, ml_ref, 0)
    w_ref[:, pl.ds(pl.multiple_of((1 - core) * width, width), width)] = product(u, oh_ref, ol_ref, 0)
    return w_ref[...]


def second_kernel(u_ref, ends_ref, mh_ref, ml_ref, oh_ref, ol_ref, mix_ref, out_ref, rim_ref, w_ref):
    u = u_ref[...]
    w = along_product(lax.axis_index("core"), u, mh_ref, ml_ref, oh_ref, ol_ref, w_ref)
    at = u.shape[1]
    rows = [joined([ends_ref[4 * j + k : 4 * j + k + 1, at : at + LANES] for k in range(4)]) for j in range(4)]
    keep_rims(rim_ref, rows)
    out_ref[...] = mixed(w, u, rows, mix_ref[1])


def third_kernel(u_ref, mh_ref, ml_ref, oh_ref, ol_ref, rim_ref, mix_ref, out_ref):
    width = mh_ref.shape[1]
    core = lax.axis_index("core")
    u_mine = u_ref[:, pl.ds(pl.multiple_of(core * width, width), width)]
    u_other = u_ref[:, pl.ds(pl.multiple_of((1 - core) * width, width), width)]
    w = product(u_mine, mh_ref, ml_ref, 1) + product(u_other, oh_ref, ol_ref, 1)
    rows = [rim_ref[k : k + 1, :] for k in range(4)]
    out_ref[...] = mixed(w, u_ref[...], rows, mix_ref[2])


def fourth_kernel(u_ref, mh_ref, ml_ref, oh_ref, ol_ref, rim_ref, mix_ref, out_ref, w_ref):
    u = u_ref[...]
    w = along_product(lax.axis_index("core"), u, mh_ref, ml_ref, oh_ref, ol_ref, w_ref)
    rows = [rim_ref[k : k + 1, :] for k in range(4)]
    f = mixed(w, u, rows, mix_ref[3])
    width = out_ref.shape[2]
    peers = out_ref.shape[0] // 2
    for k in range(2):
        out_ref[k * peers : (k + 1) * peers] = f[:, k * width : (k + 1) * width].reshape(peers, 8, width)


def shards(propagator, slab, fields, phonon, couplings):
    block, width = propagator.shape
    count = 2 * width
    columns = slab.T
    half = columns.shape[0] // 2
    peers = lax.axis_size(ROW)
    groups = lax.axis_size("z")
    held = peers * half

    def full(*shape):
        return jax.ShapeDtypeStruct(shape, jnp.float32)

    mine = propagator
    other = swapped(propagator, "core")

    rims = jnp.concatenate([mine[-2:].reshape(4, LANES), mine[:2].reshape(4, LANES)])
    parts = jnp.stack([jnp.concatenate([columns[k * half : (k + 1) * half], rims], axis=1) for k in range(2)])
    parts = jnp.broadcast_to(parts[:, None], (2, peers, half, width + LANES))
    g = exchanged(parts.reshape(2 * peers, half, width + LANES), PAIRED_ROW)

    mix = call(
        functools.partial(mixing_kernel, block), "mixing", full(SLICES, 8, count), [VMEM] * 3, size=4 * 10 * SITES
    )(couplings[None], phonon, fields)

    split = jax.ShapeDtypeStruct((block, width), jnp.bfloat16)
    pieces = call(split_kernel, "split", (split,) * 4, [VMEM, VMEM], size=16 * block * width)(mine, other)

    work = dict(flops=12 * held * block * count, size=8 * block * count)
    out, row_rim = call(
        first_kernel, "first", (full(groups, 2 * half, block + LANES), full(8, count)), [VMEM] * 8, **work
    )(g, mine, other, *pieces, mix)
    share = exchanged(out, "z").sum(axis=0)
    across = swapped(share, "yhi")
    u = gathered(share[:, :block] + across[:, :block], "z")

    scratch = [pltpu.VMEM((held, count), jnp.float32)]
    w, cut_rim = call(
        second_kernel, "second", (full(held, count), full(8, block)), [VMEM] * 7, scratch, **work
    )(u, across, *pieces, mix)
    u = gathered(summed(w, ROW), ROW)

    w = call(third_kernel, "third", full(held, block), [VMEM] * 7, **work)(
        u, *pieces, row_rim, mix
    )
    share = summed(w, "z")
    u = gathered(share + swapped(share, "yhi"), "z")

    parts = call(
        fourth_kernel, "fourth", full(2 * peers, half, width), [VMEM] * 7, scratch, **work
    )(u, *pieces, cut_rim, mix)
    out = exchanged(parts, PAIRED_ROW).reshape(2, peers, half, width).sum(axis=1)
    return out.reshape(2 * half, width).T


def solution(mesh):
    devices = mesh.devices.reshape(8, 2, 2, 4, 4)
    fine = Mesh(devices, ("z", "yhi", "core", "x", "ylo"))
    cuts = ("z", "yhi", "core")
    in_specs = (P(ROW, cuts), P(cuts, ROW), P(), P(), P())
    return jax.shard_map(shards, mesh=fine, in_specs=in_specs, out_specs=P(cuts, ROW), check_vma=False)
```

```python
import functools

import jax
import jax.numpy as jnp
from jax import lax
from jax.experimental import pallas as pl
from jax.experimental.pallas import tpu as pltpu
from jax.sharding import Mesh, PartitionSpec as P

SITES = 8192
SLICES = 4
LEVELS = 16
LANES = 128

hs_strength = 0.3

ROW = ("x", "ylo")
CUT = ("z", "yhi")
PAIRED_ROW = ("core", "x", "ylo")

VMEM = pl.BlockSpec(memory_space=pltpu.VMEM)


def swapped(x, axis):
    return lax.ppermute(x, axis, [(0, 1), (1, 0)])


def exchanged(parts, axes):
    return lax.all_to_all(parts, axes, 0, 0, tiled=True)


def gathered(x, axes):
    count = lax.axis_size(axes)
    parts = exchanged(jnp.broadcast_to(x[None], (count, *x.shape)), axes)
    return parts.reshape(count * x.shape[0], x.shape[1])


def summed(x, axes):
    count = lax.axis_size(axes)
    return exchanged(x.reshape(count, x.shape[0] // count, x.shape[1]), axes).sum(axis=0)


def call(kernel, name, out_shape, in_specs, scratch=(), flops=0, size=0):
    return pl.pallas_call(
        kernel,
        out_shape=out_shape,
        in_specs=in_specs,
        out_specs=jax.tree.map(lambda _: VMEM, out_shape),
        scratch_shapes=list(scratch),
        compiler_params=pltpu.CompilerParams(vmem_limit_bytes=24 * 1024 * 1024),
        cost_estimate=pl.CostEstimate(flops=flops, bytes_accessed=size, transcendentals=0),
        name=name,
    )


def place(axes):
    at = 0
    for axis in axes:
        at = at * lax.axis_size(axis) + lax.axis_index(axis)
    return at


def mixing_kernel(block, couplings_ref, phonon_ref, fields_ref, out_ref):
    count = out_ref.shape[2]
    for turn in range(2):
        first = place(ROW) * block if turn == 0 else place(CUT) * count
        at_before = pl.ds(pl.multiple_of((first + (SITES - LANES)) % SITES, LANES), LANES)
        at_block = pl.ds(pl.multiple_of(first, LANES), count)
        at_after = pl.ds(pl.multiple_of((first + count) % SITES, LANES), LANES)
        level = jnp.concatenate([phonon_ref[:, at_before], phonon_ref[:, at_block], phonon_ref[:, at_after]], axis=1)
        rate = jnp.zeros(level.shape, jnp.float32)
        for k in range(LEVELS):
            rate = jnp.where(level == k, couplings_ref[0:1, k : k + 1], rate)
        grown, shrunk = jnp.exp(rate), jnp.exp(-rate)
        cosh, sinh = 0.5 * (grown + shrunk), 0.5 * (grown - shrunk)
        cosh_left, sinh_left = pltpu.roll(cosh, 1, 1), pltpu.roll(sinh, 1, 1)
        even = lax.broadcasted_iota(jnp.int32, rate.shape, 1) % 2 == 0
        inside = slice(LANES, LANES + count)
        sign = (2 * fields_ref[:, at_block] - 1).astype(jnp.float32)
        scale = jnp.exp(hs_strength * sign)
        rows = [
            jnp.where(even, cosh, cosh_left)[:, inside],
            jnp.where(even, sinh, sinh_left)[:, inside],
            scale * jnp.where(even, cosh_left, cosh)[:, inside],
            scale * jnp.where(even, sinh_left, sinh)[:, inside],
            jnp.concatenate(
                [cosh[:, :LANES], cosh[:, LANES + count :], sinh[:, :LANES], sinh[:, LANES + count :]], axis=1
            ),
        ]
        for slice_no in range(turn, SLICES, 2):
            for k, row in enumerate(rows):
                out_ref[slice_no, k : k + 1, :] = row[slice_no : slice_no + 1]


def halves(x):
    high = x.astype(jnp.bfloat16)
    return high, (x - high.astype(jnp.float32)).astype(jnp.bfloat16)


def split_kernel(mine_ref, other_ref, *out_refs):
    for k, ref in enumerate((mine_ref, other_ref)):
        out_refs[2 * k][...], out_refs[2 * k + 1][...] = halves(ref[...])


def product(a, b_high_ref, b_low_ref, contract_b):
    dims = (((1,), (contract_b,)), ((), ()))
    dot = functools.partial(lax.dot_general, dimension_numbers=dims, preferred_element_type=jnp.float32)
    a_high, a_low = halves(a)
    both = dot(jnp.concatenate([a_high, a_low], axis=0), b_high_ref[...])
    count = a.shape[0]
    return both[:count] + (both[count:] + dot(a_high, b_low_ref[...]))


def mixed(w, u, rim, mix):
    before, after = LANES - 2, LANES
    rim_left = mix[4:5, before + 2 * LANES : before + 2 * LANES + 1] * rim[0] + mix[4:5, before : before + 1] * rim[1]
    rim_right = mix[4:5, after : after + 1] * rim[2] + mix[4:5, after + 2 * LANES : after + 2 * LANES + 1] * rim[3]
    end_left = jnp.sum(u * rim_left, axis=1, keepdims=True)
    end_right = jnp.sum(u * rim_right, axis=1, keepdims=True)
    count = w.shape[1]
    lane = lax.broadcasted_iota(jnp.int32, w.shape, 1)
    even = lane % 2 == 0
    partner = jnp.where(even, pltpu.roll(w, count - 1, 1), pltpu.roll(w, 1, 1))
    e = mix[0:1] * w + mix[1:2] * partner
    below = jnp.where(lane == 0, end_left, pltpu.roll(e, 1, 1))
    above = jnp.where(lane == count - 1, end_right, pltpu.roll(e, count - 1, 1))
    return mix[2:3] * e + mix[3:4] * jnp.where(even, below, above)


def joined(pieces):
    return jnp.concatenate(pieces, axis=1)


def in_rows(x, row):
    return [x[row : row + 1, k * LANES : (k + 1) * LANES] for k in range(x.shape[1] // LANES)]


def keep_rims(ref, rows):
    ref[...] = jnp.zeros(ref.shape, ref.dtype)
    for k, row in enumerate(rows):
        ref[k : k + 1, :] = row


def first_kernel(g_ref, mine_ref, other_ref, mh_ref, ml_ref, oh_ref, ol_ref, mix_ref, out_ref, rim_ref):
    core, row, z, high = lax.axis_index("core"), place(ROW), lax.axis_index("z"), lax.axis_index("yhi")
    peers = g_ref.shape[0] // 2
    width = mine_ref.shape[1]
    columns = peers * g_ref.shape[1]

    def of_core(k):
        return g_ref[pl.ds(k * peers, peers), :, 0:width].reshape(columns, width)

    w = product(of_core(core), mh_ref, ml_ref, 1) + product(of_core(1 - core), oh_ref, ol_ref, 1)
    u = joined([of_core(0), of_core(1)])
    low, top = [], []
    for k in range(2):
        low.append(g_ref[k * peers + (row + peers - 1) % peers, :, width : width + LANES])
        top.append(g_ref[k * peers + (row + 1) % peers, :, width : width + LANES])
    rows = [
        joined([tile[2 * j + i : 2 * j + i + 1] for tile in tiles for i in range(2)])
        for tiles, start in ((low, 0), (top, 2))
        for j in (start, start + 1)
    ]
    keep_rims(rim_ref, rows)
    groups = out_ref.shape[0]
    out_ref[:, :, 0 : w.shape[1]] = mixed(w, u, rows, mix_ref[0]).reshape(groups, columns // groups, w.shape[1])

    upper = jnp.where(core == 1, mine_ref[:, width - LANES :], other_ref[:, width - LANES :]).T
    lower = jnp.where(core == 0, mine_ref[:, :LANES], other_ref[:, :LANES]).T
    tail = jnp.concatenate(in_rows(upper, LANES - 2) + in_rows(upper, LANES - 1), axis=0)
    head = jnp.concatenate(in_rows(lower, 0) + in_rows(lower, 1), axis=0)
    tail_to = (z + high) % groups
    head_to = (z + groups - 1 + high) % groups
    for p in range(groups):
        out_ref[p, 0:8, w.shape[1] :] = jnp.where(tail_to == p, tail, 0.0)
        out_ref[p, 8:16, w.shape[1] :] = jnp.where(head_to == p, head, 0.0)


def along_product(core, u, mh_ref, ml_ref, oh_ref, ol_ref, w_ref):
    width = mh_ref.shape[1]
    w_ref[:, pl.ds(pl.multiple_of(core * width, width), width)] = product(u, mh_ref, ml_ref, 0)
    w_ref[:, pl.ds(pl.multiple_of((1 - core) * width, width), width)] = product(u, oh_ref, ol_ref, 0)
    return w_ref[...]


def second_kernel(u_ref, ends_ref, mh_ref, ml_ref, oh_ref, ol_ref, mix_ref, out_ref, rim_ref, w_ref):
    u = u_ref[...]
    w = along_product(lax.axis_index("core"), u, mh_ref, ml_ref, oh_ref, ol_ref, w_ref)
    at = u.shape[1]
    rows = [joined([ends_ref[4 * j + k : 4 * j + k + 1, at : at + LANES] for k in range(4)]) for j in range(4)]
    keep_rims(rim_ref, rows)
    out_ref[...] = mixed(w, u, rows, mix_ref[1])


def third_kernel(u_ref, mh_ref, ml_ref, oh_ref, ol_ref, rim_ref, mix_ref, out_ref):
    width = mh_ref.shape[1]
    core = lax.axis_index("core")
    u_mine = u_ref[:, pl.ds(pl.multiple_of(core * width, width), width)]
    u_other = u_ref[:, pl.ds(pl.multiple_of((1 - core) * width, width), width)]
    w = product(u_mine, mh_ref, ml_ref, 1) + product(u_other, oh_ref, ol_ref, 1)
    rows = [rim_ref[k : k + 1, :] for k in range(4)]
    out_ref[...] = mixed(w, u_ref[...], rows, mix_ref[2])


def fourth_kernel(u_ref, mh_ref, ml_ref, oh_ref, ol_ref, rim_ref, mix_ref, out_ref, w_ref):
    u = u_ref[...]
    w = along_product(lax.axis_index("core"), u, mh_ref, ml_ref, oh_ref, ol_ref, w_ref)
    rows = [rim_ref[k : k + 1, :] for k in range(4)]
    f = mixed(w, u, rows, mix_ref[3])
    width = out_ref.shape[2]
    peers = out_ref.shape[0] // 2
    for k in range(2):
        out_ref[k * peers : (k + 1) * peers] = f[:, k * width : (k + 1) * width].reshape(peers, 8, width)


def shards(propagator, slab, fields, phonon, couplings):
    block, width = propagator.shape
    count = 2 * width
    columns = slab.T
    half = columns.shape[0] // 2
    peers = lax.axis_size(ROW)
    groups = lax.axis_size("z")
    held = peers * half

    def full(*shape):
        return jax.ShapeDtypeStruct(shape, jnp.float32)

    mine = propagator
    other = swapped(propagator, "core")

    rims = jnp.concatenate([mine[-2:].reshape(4, LANES), mine[:2].reshape(4, LANES)])
    parts = jnp.stack([jnp.concatenate([columns[k * half : (k + 1) * half], rims], axis=1) for k in range(2)])
    parts = jnp.broadcast_to(parts[:, None], (2, peers, half, width + LANES))
    g = exchanged(parts.reshape(2 * peers, half, width + LANES), PAIRED_ROW)

    mix = call(
        functools.partial(mixing_kernel, block), "mixing", full(SLICES, 8, count), [VMEM] * 3, size=4 * 10 * SITES
    )(couplings[None], phonon, fields)

    split = jax.ShapeDtypeStruct((block, width), jnp.bfloat16)
    pieces = call(split_kernel, "split", (split,) * 4, [VMEM, VMEM], size=16 * block * width)(mine, other)

    work = dict(flops=12 * held * block * count, size=8 * block * count)
    out, row_rim = call(
        first_kernel, "first", (full(groups, 2 * half, block + LANES), full(8, count)), [VMEM] * 8, **work
    )(g, mine, other, *pieces, mix)
    share = exchanged(out, "z").sum(axis=0)
    across = swapped(share, "yhi")
    u = gathered(share[:, :block] + across[:, :block], "z")

    scratch = [pltpu.VMEM((held, count), jnp.float32)]
    w, cut_rim = call(
        second_kernel, "second", (full(held, count), full(8, block)), [VMEM] * 7, scratch, **work
    )(u, across, *pieces, mix)
    u = gathered(summed(w, ROW), ROW)

    w = call(third_kernel, "third", full(held, block), [VMEM] * 7, **work)(
        u, *pieces, row_rim, mix
    )
    share = summed(w, "z")
    u = gathered(share, CUT).reshape(groups, 2, 2 * half, block).sum(axis=1).reshape(held, block)

    parts = call(
        fourth_kernel, "fourth", full(2 * peers, half, width), [VMEM] * 7, scratch, **work
    )(u, *pieces, cut_rim, mix)
    out = exchanged(parts, PAIRED_ROW).reshape(2, peers, half, width).sum(axis=1)
    return out.reshape(2 * half, width).T


def solution(mesh):
    devices = mesh.devices.reshape(8, 2, 2, 4, 4)
    fine = Mesh(devices, ("z", "yhi", "core", "x", "ylo"))
    cuts = ("z", "yhi", "core")
    in_specs = (P(ROW, cuts), P(cuts, ROW), P(), P(), P())
    return jax.shard_map(shards, mesh=fine, in_specs=in_specs, out_specs=P(cuts, ROW), check_vma=False)
```
